256 devices in a mesh: grp: 2 (over y), aux: 16 (over z), orb: 4 (over x), occ: 2 (over core).
Axes of the slice: x: 4, y: 2, z: 16, core: 2. Of those that a mesh axis runs over, the one named last changes fastest.
The devices are a block of a 4x16x16 slice.
Arguments:
- b_tiles: bfloat16 [256, 32, 4, 128, 128], P(('grp', 'aux'), 'orb'), parts along dimension 0, may hold values from -0.25 to 0.25
- nu_block: int32 [256, 32, 4], P(('grp', 'aux'), 'orb'), parts along dimension 0, may hold values from 0 to 31
- tile_mask: int32 [256, 32, 4], P(('grp', 'aux'), 'orb'), parts along dimension 0, may hold values 0 or 1
- assignment: int32 [256], P(('grp', 'aux')), parts along dimension 0, may hold values from 0 to 127, each once
- metric_factor: float32 [256], P('grp'), parts along dimension 0, may hold values from 0.05 to 0.3
- orbitals: bfloat16 [800, 4000], P('grp'), parts along dimension 0, may hold values from -6 to 6
- occupied_index: int32 [64], P(('grp', 'occ')), parts along dimension 0, may hold values from 0 to 399
Outputs:
- exchange: float32 [8192, 4096], P(('grp', 'aux', 'occ'), 'orb'), parts along dimension 0
The draws below stay inside these ranges and needn't reach their ends.
There are 2 independent parts, one for each index of `grp`. The reference program is written for one: setup_inputs(seed, part) draws one part's arguments, and reference() takes and returns one part's arrays. A program takes and returns all parts, laid end to end along the dimension named above; each array names one. Nothing has to cross between parts.
Inputs may be any that keep to these rules, and one draw needn't show every extreme that they name: `nu_block`: each entry names a column block. `assignment`: each number once. `occupied_index`: repeats may occur.
All inputs are finite; a program needn't handle non-finite values. No bound on the sum of `tile_mask` on one device may be relied on, other than what follows from the above.
Results may differ from the reference program's by a relative error of at most 0.0033.
Values may be sent and summed in bfloat16 or wider, within the bound.
No kernel may reach another device: no remote copies, remote signals or barrier semaphores. Data moves between devices by JAX's collectives and lax.ppermute only.
A program may use at most 128 MiB of HBM per device.

```python
import math
import jax
import jax.numpy as jnp
from jax import lax

N = 4000
TILE = 128
NOCC = 400
BATCH = 32
SLOTS = 4
NB = 32
NAUX = 128


def touch_ends(result, key, smallest, largest):
    spot = [jax.random.randint(jax.random.fold_in(key, axis), (), 0, length) for axis, length in enumerate(result.shape)]
    widest = result.shape.index(max(result.shape))
    neighbour = spot[:widest] + [(spot[widest] + 1) % result.shape[widest]] + spot[widest + 1:]
    return result.at[tuple(spot)].set(smallest).at[tuple(neighbour)].set(largest)


def levels(own_key, dims, cuts, smallest, largest):
    level = 1.0
    for axis_at, shards_of in cuts:
        steps = jax.random.uniform(jax.random.fold_in(jax.random.fold_in(own_key, 6), axis_at), (shards_of,), jnp.float32, smallest / len(cuts), largest / len(cuts))
        level = level * jnp.repeat(jnp.exp(steps), dims[axis_at] // shards_of).reshape((-1,) + (1,) * (len(dims) - 1 - axis_at))
    return level


def gaussian(stream_key, dims, deviation, reach, cuts=(), held_as=jnp.bfloat16):
    factor_of = levels(stream_key, dims, cuts, -0.22, 0.18) if cuts else 1.0
    array = jax.random.normal(stream_key, dims, jnp.float32) * deviation * factor_of
    return jnp.minimum(jnp.maximum(array, -reach), reach).astype(held_as)


def setup_inputs(seed: int = 0, part: int = 0) -> dict:
    arg_keys = jax.random.split(jax.random.key(seed), 8)
    part_splits = jax.random.split(jax.random.fold_in(arg_keys[7], part), 8)
    return {
        "b_tiles": gaussian(part_splits[0], (NAUX, NB, SLOTS, TILE, TILE), (SLOTS * TILE) ** -0.5, 0.25, ((0, 16), (1, 4))),
        "nu_block": touch_ends(jax.random.randint(part_splits[1], (NAUX, NB, SLOTS), 0, NB), jax.random.fold_in(part_splits[1], 1), 0, NB - 1).astype(jnp.int32),
        "tile_mask": touch_ends((jax.random.randint(part_splits[2], (NAUX, NB, SLOTS), 0, 4) < 3).astype(jnp.int32), jax.random.fold_in(part_splits[2], 1), 0, 1),
        "assignment": jax.random.permutation(part_splits[3], NAUX).astype(jnp.int32),
        "metric_factor": jnp.clip(jnp.exp(jax.random.uniform(part_splits[4], (NAUX,), jnp.float32, math.log(0.05), math.log(0.3))), 0.05, 0.3),
        "orbitals": gaussian(part_splits[5], (NOCC, N), 1.0, 6.0),
        "occupied_index": touch_ends(jax.random.randint(part_splits[6], (BATCH,), 0, NOCC), jax.random.fold_in(part_splits[6], 1), 0, NOCC - 1).astype(jnp.int32),
    }


def reference(b_tiles, nu_block, tile_mask, assignment, metric_factor, orbitals, occupied_index):
    nblocks = (N + TILE - 1) // TILE
    padded = nblocks * TILE
    picked = orbitals[occupied_index].astype(jnp.float32)
    picked = jnp.pad(picked, ((0, 0), (0, padded - N)))
    blocks = picked.reshape(BATCH, nblocks, TILE)
    factors = metric_factor[assignment]
    inside = jnp.arange(padded) < N

    def half_transform(inputs):
        stored, columns, masking, scaled = inputs
        chosen = blocks[:, columns] * masking.astype(jnp.float32)[None, :, :, None]
        product = jnp.einsum("msab,imsb->ima", stored.astype(jnp.float32), chosen, precision=lax.Precision.HIGHEST)
        product = product.reshape(BATCH, padded) * scaled
        return jnp.where(inside[None, :], product, 0.0).astype(jnp.bfloat16)

    slab_list = lax.map(half_transform, (b_tiles, nu_block, tile_mask, factors))
    flattened = slab_list.reshape(-1, padded).astype(jnp.float32)
    return lax.dot_general(flattened, flattened, (((0,), (0,)), ((), ())), precision=lax.Precision.HIGHEST)
```

```python
import functools

import jax
import jax.numpy as jnp
from jax import lax
from jax.experimental import pallas as pl
from jax.experimental.pallas import tpu as pltpu
from jax.sharding import PartitionSpec as P


def accumulate_kernel(counts, has_prev, place_ref, *refs):
    nb = len(counts)
    n = sum(counts)
    row_refs = refs[: 4 * nb]
    half_refs = refs[4 * nb : 4 * nb + 2 * n]
    rest = refs[4 * nb + 2 * n :]
    prev, outs = (rest[:2], rest[2:]) if has_prev else (None, rest)
    is_root = place_ref[0] == 0
    core = place_ref[1]
    mine = outs[0].shape[0]
    rows = []
    for b in range(nb):
        own, *others = row_refs[4 * b : 4 * b + 4]
        for j in range(counts[b]):
            for_out = []
            for side in range(2):
                which = core if side == 0 else 1 - core
                at = pl.ds(pl.multiple_of(j * 2 * mine + which * mine, mine), mine)
                got = others[0][at, :] + others[1][at, :] + others[2][at, :]
                for_out.append(jnp.where(is_root, own[at, :], got))
            rows.append(for_out)
    half = half_refs[0].shape[0]
    step = 256
    for h in range(2):
        for c in range(half // step):
            for side in range(2):
                at = pl.ds(h * half + c * step, step)
                acc = prev[side][:, at] if has_prev else None
                for j in range(0, n, 2):
                    js = range(j, min(j + 2, n))
                    left = jnp.concatenate([rows[k][side] for k in js], axis=1)
                    right = jnp.concatenate(
                        [half_refs[2 * k + h][c * step : (c + 1) * step, :] for k in js], axis=1
                    )
                    part = lax.dot_general(
                        left, right, (((1,), (1,)), ((), ())), preferred_element_type=jnp.float32
                    )
                    acc = part if acc is None else acc + part
                outs[side][:, at] = acc


def accumulate(place, batches, slabs, prev, block_rows, columns):
    counts = tuple(len(s) for s in slabs)
    has_prev = prev is not None
    operands = [x for b in batches for x in b]
    operands += [h for s in slabs for pair in s for h in pair]
    operands += list(prev) if has_prev else []
    vmem = pl.BlockSpec(memory_space=pltpu.VMEM)
    flops = 2 * 2 * block_rows * columns * sum(counts) * slabs[0][0][0].shape[1]
    return pl.pallas_call(
        functools.partial(accumulate_kernel, counts, has_prev),
        out_shape=[jax.ShapeDtypeStruct((block_rows, columns), jnp.float32)] * 2,
        in_specs=[pl.BlockSpec(memory_space=pltpu.SMEM)] + [vmem] * len(operands),
        out_specs=[vmem] * 2,
        cost_estimate=pl.CostEstimate(flops=flops, bytes_accessed=0, transcendentals=0),
        name="accumulate",
    )(place, *operands)


def per_device(b_tiles, nu_block, tile_mask, assignment, metric_factor, orbitals, occupied_index):
    naux_dev, row_blocks = b_tiles.shape[0], b_tiles.shape[1]
    tile_size = b_tiles.shape[3]
    n_basis = orbitals.shape[1]
    nblocks = (n_basis + tile_size - 1) // tile_size
    padded = nblocks * tile_size
    mu_dev = row_blocks * tile_size
    batch_dev = occupied_index.shape[0]
    n_aux, n_orb, n_occ = lax.axis_size("aux"), lax.axis_size("orb"), lax.axis_size("occ")
    z, x, core = lax.axis_index("aux"), lax.axis_index("orb"), lax.axis_index("occ")

    picked = jnp.take(orbitals, occupied_index, axis=0)
    picked = jnp.pad(picked, ((0, 0), (0, padded - n_basis)))
    blocks = picked.reshape(batch_dev, nblocks, tile_size)
    chosen = blocks[:, nu_block] * tile_mask.astype(jnp.bfloat16)[None, :, :, :, None]
    half_product = jnp.einsum(
        "pmsab,ipmsb->mapi", b_tiles, chosen, preferred_element_type=jnp.float32
    )
    lookup_table = (
        assignment[:, None] == jnp.arange(metric_factor.shape[0], dtype=jnp.int32)[None, :]
    ).astype(jnp.float32)
    factors = jnp.dot(lookup_table, metric_factor, precision=lax.Precision.HIGHEST)
    row_index = x * mu_dev + jnp.arange(mu_dev, dtype=jnp.int32)
    scaled = half_product.reshape(mu_dev, naux_dev, batch_dev) * factors[None, :, None]
    scaled = jnp.where(row_index[:, None, None] < n_basis, scaled, 0.0)
    slab = scaled.astype(jnp.bfloat16).reshape(mu_dev, naux_dev * batch_dev)

    block_rows = padded // (n_aux * n_occ)
    plane_rows = block_rows * n_occ
    per_orb = mu_dev // plane_rows
    half = mu_dev // 2
    per_half = half // plane_rows
    root = z // per_orb
    rel = lax.rem(x - root + n_orb, n_orb)
    in_half = lax.rem(z, per_half) * plane_rows
    upper = lax.rem(z, per_orb) >= per_half

    halves = (slab[:half], slab[half:])
    swap = [(0, 1), (1, 0)]
    theirs = tuple(lax.ppermute(h, "occ", swap) for h in halves)
    ring = [(2 * i, 2 * ((i + 1) % n_aux)) for i in range(n_aux)]
    ring += [(2 * i + 1, 2 * ((i - 1) % n_aux) + 1) for i in range(n_aux)]

    def forward(pair):
        return tuple(lax.ppermute(h, ("aux", "occ"), ring) for h in pair)

    def within(source, target):
        return [
            (i * n_orb + (i // per_orb + source) % n_orb, i * n_orb + (i // per_orb + target) % n_orb)
            for i in range(n_aux)
        ]

    def rows_of(pairs):
        own = jnp.concatenate(
            [
                lax.dynamic_slice_in_dim(jnp.where(upper, p[1], p[0]), in_half, plane_rows, 0)
                for p in pairs
            ]
        )
        axes = ("aux", "orb")
        first = lax.ppermute(own, axes, within(0, 1))
        last = lax.ppermute(own, axes, within(0, 3))
        middle = lax.ppermute(first, axes, within(1, 2))
        return own, first, middle, last

    place = jnp.stack([rel, core]).astype(jnp.int32)
    steps = n_aux // 2
    a, b = halves, theirs
    got = [[a]]
    for t in range(1, steps + 1):
        a = forward(a)
        if t < steps:
            b = forward(b)
            got.append([a, b])
        else:
            got.append([a])
    groups = [[s for t in r for s in got[t]] for r in (range(0, 4), range(4, 6), (6,), (7,), (8,))]
    rows = [rows_of(g) for g in groups]
    partial = accumulate(place, rows[:2], groups[:2], None, block_rows, mu_dev)
    mine, other = accumulate(place, rows[2:], groups[2:], partial, block_rows, mu_dev)
    return mine + lax.ppermute(other, "occ", swap)


def solution(mesh):
    in_specs = (
        P(("grp", "aux"), "orb", None, None, None),
        P(("grp", "aux"), "orb", None),
        P(("grp", "aux"), "orb", None),
        P(("grp", "aux")),
        P("grp"),
        P("grp", None),
        P(("grp", "occ")),
    )
    out_specs = P(("grp", "aux", "occ"), "orb")
    return jax.shard_map(
        per_device, mesh=mesh, in_specs=in_specs, out_specs=out_specs, check_vma=False
    )
```

```python
import functools

import jax
import jax.numpy as jnp
from jax import lax
from jax.experimental import pallas as pl
from jax.experimental.pallas import tpu as pltpu
from jax.sharding import PartitionSpec as P


VMEM_BYTES = 12 * 1024 * 1024
TRANSFORM_VMEM_BYTES = 60 * 1024 * 1024
STAGE_FLOPS = 2_000_000_000


def contract_last(left, right):
    return lax.dot_general(
        left, right, (((1,), (1,)), ((), ())), preferred_element_type=jnp.float32
    )


def transform_kernel(
    build, n_basis, block0, place_ref, index_ref, nu_ref, mask_ref, assign_ref, metric_ref,
    table_or_orbitals_ref, tiles_ref, out_ref, *rest
):
    n_p, _, slots, tile, _ = tiles_ref.shape
    lanes = out_ref.shape[1]
    n_i = lanes // n_p
    step = pl.program_id(0)
    if build:
        table_ref, lane_mask_ref, rows_ref, sem = rest
    else:
        table_ref = table_or_orbitals_ref
        (lane_mask_ref,) = rest
    blocks = table_ref.shape[0] // tile - 1

    @pl.when(step == 0)
    def _():
        lane = lax.broadcasted_iota(jnp.int32, (16, lanes), 1)
        for p in range(n_p):
            lane_mask_ref[p] = jnp.where(lane // n_i == p, 1.0, 0.0).astype(jnp.bfloat16)
        if build:
            group = rows_ref.shape[1]
            for i in range(n_i):
                at = pl.ds(pl.multiple_of(index_ref[i] // group * group, group), group)
                pltpu.make_async_copy(
                    table_or_orbitals_ref.at[at, :], rows_ref.at[i], sem.at[i]
                ).start()
            row = lax.broadcasted_iota(jnp.int32, (n_i * group, lanes), 0)
            col = lax.broadcasted_iota(jnp.int32, (n_i * group, lanes), 1)
            wanted = jnp.zeros((n_i * group, lanes), jnp.int32)
            for i in range(n_i):
                wanted = jnp.where(col % n_i == i, i * group + index_ref[i] % group, wanted)
            one_hot = jnp.where(row == wanted, 1.0, 0.0).astype(jnp.bfloat16)
            for i in range(n_i):
                pltpu.make_async_copy(
                    table_or_orbitals_ref.at[pl.ds(0, group), :], rows_ref.at[i], sem.at[i]
                ).wait()
            table_ref[pl.ds((blocks - 1) * tile, 2 * tile), :] = jnp.zeros(
                (2 * tile, lanes), jnp.bfloat16
            )
            for k in range(blocks):
                wide = min(tile, n_basis - k * tile)
                got = rows_ref[:, :, k * tile : k * tile + wide].reshape(n_i * group, wide)
                turned = lax.dot_general(
                    got, one_hot, (((0,), (0,)), ((), ())), preferred_element_type=jnp.float32
                )
                table_ref[k * tile : k * tile + wide, :] = turned.astype(jnp.bfloat16)

    total = jnp.zeros((tile, lanes), jnp.float32)
    for p in range(n_p):
        lane_mask = lane_mask_ref[p]
        for s in range(0, slots, 2):
            weights = []
            for t in (s, s + 1):
                nu = jnp.where(mask_ref[p, t, block0 + step] > 0, nu_ref[p, t, block0 + step], blocks)
                part = table_ref[pl.ds(pl.multiple_of(nu * tile, tile), tile), :]
                part = part.reshape(tile // 16, 16, lanes) * lane_mask[None]
                weights.append(part.reshape(tile, lanes))
            left = jnp.concatenate([tiles_ref[p, 0, s], tiles_ref[p, 0, s + 1]], axis=1)
            total = total + jnp.dot(
                left, jnp.concatenate(weights, axis=0), preferred_element_type=jnp.float32
            )
    lane = lax.broadcasted_iota(jnp.int32, (1, lanes), 1)
    factors = jnp.zeros((1, lanes), jnp.float32)
    for p in range(n_p):
        factors = jnp.where(lane // n_i == p, metric_ref[assign_ref[p]], factors)
    row = place_ref[2] + (block0 + step) * tile + lax.broadcasted_iota(jnp.int32, (tile, lanes), 0)
    out_ref[...] = jnp.where(row < n_basis, total * factors, 0.0).astype(out_ref.dtype)


def transform(build, block0, n_blocks, n_basis, scalars, table, b_tiles):
    n_p, _, slots, tile, _ = b_tiles.shape
    n_i = scalars[1].shape[0]
    lanes = n_p * n_i
    blocks = (n_basis + tile - 1) // tile
    smem = pl.BlockSpec(memory_space=pltpu.SMEM)
    vmem = pl.BlockSpec(memory_space=pltpu.VMEM)
    table_shape = jax.ShapeDtypeStruct(((blocks + 1) * tile, lanes), jnp.bfloat16)
    out_shape = [jax.ShapeDtypeStruct((n_blocks * tile, lanes), jnp.bfloat16)]
    out_specs = [pl.BlockSpec((tile, lanes), lambda m: (m, 0))]
    scratch = [pltpu.VMEM((n_p, 16, lanes), jnp.bfloat16)]
    if build:
        out_shape.append(table_shape)
        out_specs.append(vmem)
        scratch += [
            pltpu.VMEM((n_i, 8, n_basis), jnp.bfloat16),
            pltpu.SemaphoreType.DMA((n_i,)),
        ]
    return pl.pallas_call(
        functools.partial(transform_kernel, build, n_basis, block0),
        grid=(n_blocks,),
        out_shape=out_shape,
        in_specs=[smem] * len(scalars)
        + [pl.BlockSpec(memory_space=pl.ANY) if build else vmem]
        + [pl.BlockSpec((n_p, 1, slots, tile, tile), lambda m: (0, block0 + m, 0, 0, 0))],
        out_specs=out_specs,
        scratch_shapes=scratch,
        compiler_params=pltpu.CompilerParams(vmem_limit_bytes=TRANSFORM_VMEM_BYTES),
        cost_estimate=pl.CostEstimate(
            flops=2 * n_blocks * n_p * slots * tile * tile * lanes,
            bytes_accessed=2 * n_blocks * n_p * slots * tile * tile,
            transcendentals=0,
        ),
        name="transform_first" if build else "transform_rest",
    )(*scalars, table, b_tiles)


def stage_kernel(place_ref, *refs):
    *halves, came, out_ref = refs
    count = out_ref.shape[0] // 2

    @pl.when(place_ref[0] == 0)
    def _():
        at = pl.ds(pl.multiple_of(place_ref[3], count), count)
        for k in range(2):
            low, high = halves[2 * k], halves[2 * k + 1]

            @pl.when(place_ref[4] == 0)
            def _():
                out_ref[k * count : (k + 1) * count, :] = low[at, :]

            @pl.when(place_ref[4] != 0)
            def _():
                out_ref[k * count : (k + 1) * count, :] = high[at, :]

    @pl.when(place_ref[0] != 0)
    def _():
        out_ref[...] = came[...]


def stage(place, pair, came, rows):
    vmem = pl.BlockSpec(memory_space=pltpu.VMEM)
    operands = [h for s in pair for h in s] + [came]
    return pl.pallas_call(
        stage_kernel,
        out_shape=jax.ShapeDtypeStruct((2 * rows, pair[0][0].shape[1]), pair[0][0].dtype),
        in_specs=[pl.BlockSpec(memory_space=pltpu.SMEM)] + [vmem] * len(operands),
        out_specs=vmem,
        compiler_params=pltpu.CompilerParams(vmem_limit_bytes=VMEM_BYTES),
        cost_estimate=pl.CostEstimate(flops=STAGE_FLOPS, bytes_accessed=0, transcendentals=0),
        name="stage",
    )(place, *operands)


def accumulate_kernel(n, has_prev, place_ref, *refs):
    pairs = [refs[8 * j : 8 * j + 8] for j in range(n)]
    rest = refs[8 * n :]
    prev, outs = (rest[:2], rest[2:]) if has_prev else (None, rest)
    link, core = place_ref[0], place_ref[1]
    mine = outs[0].shape[0]
    rows = []
    for j in range(n):
        both = []
        for side in range(2):
            which = core if side == 0 else 1 - core
            cut = []
            for k in range(2):
                at = pl.ds(pl.multiple_of(k * 2 * mine + which * mine, mine), mine)
                c = [r[at, :] for r in pairs[j][:4]]
                cut.append(
                    jnp.where(
                        link < 2, jnp.where(link == 0, c[0], c[1]), jnp.where(link == 2, c[2], c[3])
                    )
                )
            both.append(jnp.concatenate(cut, axis=1))
        rows.append(both)
    half = pairs[0][4].shape[0]
    step = 256
    for h in range(2):
        for c in range(half // step):
            cut = slice(c * step, (c + 1) * step)
            right = [jnp.concatenate([p[4 + h][cut, :], p[6 + h][cut, :]], axis=1) for p in pairs]
            for side in range(2):
                at = pl.ds(h * half + c * step, step)
                acc = prev[side][:, at] if has_prev else None
                for j in range(n):
                    part = contract_last(rows[j][side], right[j])
                    acc = part if acc is None else acc + part
                outs[side][:, at] = acc


def accumulate(place, candidates, pairs, prev, block_rows, columns):
    n = len(pairs)
    has_prev = prev is not None
    operands = []
    for c, pair in zip(candidates, pairs, strict=True):
        operands += list(c) + [pair[0][0], pair[0][1], pair[1][0], pair[1][1]]
    operands += list(prev) if has_prev else []
    vmem = pl.BlockSpec(memory_space=pltpu.VMEM)
    flops = 2 * 2 * block_rows * columns * 2 * n * pairs[0][0][0].shape[1]
    return pl.pallas_call(
        functools.partial(accumulate_kernel, n, has_prev),
        out_shape=[jax.ShapeDtypeStruct((block_rows, columns), jnp.float32)] * 2,
        in_specs=[pl.BlockSpec(memory_space=pltpu.SMEM)] + [vmem] * len(operands),
        out_specs=[vmem] * 2,
        compiler_params=pltpu.CompilerParams(vmem_limit_bytes=VMEM_BYTES),
        cost_estimate=pl.CostEstimate(flops=flops, bytes_accessed=0, transcendentals=0),
        name="accumulate",
    )(place, *operands)


def per_device(b_tiles, nu_block, tile_mask, assignment, metric_factor, orbitals, occupied_index):
    row_blocks, tile_size = b_tiles.shape[1], b_tiles.shape[3]
    n_basis = orbitals.shape[1]
    padded = (n_basis + tile_size - 1) // tile_size * tile_size
    mu_dev = row_blocks * tile_size
    n_aux, n_orb, n_occ = lax.axis_size("aux"), lax.axis_size("orb"), lax.axis_size("occ")
    z, x, core = lax.axis_index("aux"), lax.axis_index("orb"), lax.axis_index("occ")
    block_rows = padded // (n_aux * n_occ)
    plane_rows = block_rows * n_occ
    per_orb = mu_dev // plane_rows
    half = mu_dev // 2
    per_half = half // plane_rows

    root = z // per_orb
    away = x - root
    link = lax.rem(jnp.where(core == 0, away, -away) + n_orb, n_orb)
    in_half = lax.rem(z, per_half) * plane_rows
    upper = lax.rem(z, per_orb) // per_half
    place = jnp.stack([link, core, x * mu_dev, in_half, upper]).astype(jnp.int32)

    scalars = (
        place,
        occupied_index,
        nu_block.transpose(0, 2, 1),
        tile_mask.transpose(0, 2, 1),
        assignment,
        metric_factor,
    )
    low, table = transform(True, 0, row_blocks // 2, n_basis, scalars, orbitals, b_tiles)
    (high,) = transform(False, row_blocks // 2, row_blocks // 2, n_basis, scalars, table, b_tiles)

    swap = [(0, 1), (1, 0)]
    a = (low, high)
    b = tuple(lax.ppermute(h, "occ", swap) for h in a)
    ring = [(2 * i, 2 * ((i + 1) % n_aux)) for i in range(n_aux)]
    ring += [(2 * i + 1, 2 * ((i - 1) % n_aux) + 1) for i in range(n_aux)]

    def forward(pair):
        got = []
        for k in range(2):
            got.append(lax.ppermute(pair[k], ("aux", "occ"), ring))
        return tuple(got)

    def along(payload, links):
        pairs = []
        for i in range(n_aux):
            for c, sign in ((0, 1), (1, -1)):
                for source, target in links:
                    at = [(i * n_orb + (i // per_orb + sign * k) % n_orb) * 2 + c for k in (source, target)]
                    pairs.append(tuple(at))
        return lax.ppermute(payload, ("aux", "orb", "occ"), pairs)

    chain = [(k, k + 1) for k in range(n_orb - 1)]
    steps = n_aux // 2
    pairs, payloads = [], []
    came = jnp.zeros((2 * plane_rows, low.shape[1]), low.dtype)
    held = a
    for t in range(1, steps + 1):
        a = forward(a)
        pair = (held, a)
        pairs.append(pair)
        if t < steps:
            b = forward(b)
            held = b
        payloads.append(stage(place, pair, came, plane_rows))
        came = along(payloads[-1], chain)
    payloads.append(came)
    n = len(pairs)
    candidates = [payloads[j : j + 4] for j in range(n - 2)]
    two, one = payloads[n - 2], payloads[n - 1]
    candidates.append([two, one, came, along(two, [(0, 3)])])
    candidates.append([one, came, along(one, [(0, 2)]), along(one, [(0, 3)])])

    partial = None
    for lo, hi in ((0, n - 4), (n - 4, n - 3), (n - 3, n)):
        partial = accumulate(place, candidates[lo:hi], pairs[lo:hi], partial, block_rows, mu_dev)
    mine, other = partial
    return mine + lax.ppermute(other, "occ", swap)


def solution(mesh):
    in_specs = (
        P(("grp", "aux"), "orb", None, None, None),
        P(("grp", "aux"), "orb", None),
        P(("grp", "aux"), "orb", None),
        P(("grp", "aux")),
        P("grp"),
        P("grp", None),
        P(("grp", "occ")),
    )
    out_specs = P(("grp", "aux", "occ"), "orb")

    return jax.shard_map(
        per_device, mesh=mesh, in_specs=in_specs, out_specs=out_specs, check_vma=False
    )
```

```python
import functools

import jax
import jax.numpy as jnp
from jax import lax
from jax.experimental import pallas as pl
from jax.experimental.pallas import tpu as pltpu
from jax.sharding import PartitionSpec as P


VMEM_BYTES = 12 * 1024 * 1024
TRANSFORM_VMEM_BYTES = 60 * 1024 * 1024
BATCH_ENDS = (3, 6)


def contract_last(left, right):
    return lax.dot_general(
        left, right, (((1,), (1,)), ((), ())), preferred_element_type=jnp.float32
    )


def transform_kernel(
    build, n_basis, block0, index_ref, nu_ref, mask_ref, assign_ref, metric_ref,
    table_or_orbitals_ref, tiles_ref, out_ref, *rest
):
    n_p, row_blocks, slots, tile, _ = tiles_ref.shape
    lanes = out_ref.shape[1]
    n_i = lanes // n_p
    step = pl.program_id(0)
    if build:
        table_ref, lane_mask_ref, held_ref, tile_sem, rows_ref, row_sem = rest
    else:
        table_ref = table_or_orbitals_ref
        lane_mask_ref, held_ref, tile_sem = rest
    blocks = table_ref.shape[0] // tile - 1
    n_blocks = held_ref.shape[0]

    def fetch(m, p):
        return pltpu.make_async_copy(
            tiles_ref.at[p, block0 + m], held_ref.at[m, p], tile_sem.at[m, p]
        )

    @pl.when(step == 0)
    def _():
        if build:
            group = rows_ref.shape[1]

            def row_copy(i):
                at = pl.ds(pl.multiple_of(index_ref[i] // group * group, group), group)
                return pltpu.make_async_copy(
                    table_or_orbitals_ref.at[at, :], rows_ref.at[i], row_sem.at[i]
                )

            for i in range(n_i):
                row_copy(i).start()
        for m in range(n_blocks):
            for p in range(n_p):
                fetch(m, p).start()
        lane = lax.broadcasted_iota(jnp.int32, (16, lanes), 1)
        for p in range(n_p):
            lane_mask_ref[p] = jnp.where(lane // n_i == p, 1.0, 0.0).astype(jnp.bfloat16)
        if build:
            row = lax.broadcasted_iota(jnp.int32, (n_i * group, lanes), 0)
            col = lax.broadcasted_iota(jnp.int32, (n_i * group, lanes), 1)
            wanted = jnp.zeros((n_i * group, lanes), jnp.int32)
            for i in range(n_i):
                wanted = jnp.where(col % n_i == i, i * group + index_ref[i] % group, wanted)
            one_hot = jnp.where(row == wanted, 1.0, 0.0).astype(jnp.bfloat16)
            table_ref[pl.ds((blocks - 1) * tile, 2 * tile), :] = jnp.zeros(
                (2 * tile, lanes), jnp.bfloat16
            )
            for i in range(n_i):
                row_copy(i).wait()
            for k in range(blocks):
                wide = min(tile, n_basis - k * tile)
                got = rows_ref[:, :, k * tile : k * tile + wide].reshape(n_i * group, wide)
                turned = lax.dot_general(
                    got, one_hot, (((0,), (0,)), ((), ())), preferred_element_type=jnp.float32
                )
                table_ref[k * tile : k * tile + wide, :] = turned.astype(jnp.bfloat16)

    for p in range(n_p):
        fetch(step, p).wait()
    total = jnp.zeros((tile, lanes), jnp.float32)
    for p in range(n_p):
        lane_mask = lane_mask_ref[p]
        for s in range(0, slots, 2):
            weights = []
            for t in (s, s + 1):
                nu = jnp.where(mask_ref[p, t, block0 + step] > 0, nu_ref[p, t, block0 + step], blocks)
                part = table_ref[pl.ds(pl.multiple_of(nu * tile, tile), tile), :]
                part = part.reshape(tile // 16, 16, lanes) * lane_mask[None]
                weights.append(part.reshape(tile, lanes))
            left = jnp.concatenate([held_ref[step, p, s], held_ref[step, p, s + 1]], axis=1)
            total = total + jnp.dot(
                left, jnp.concatenate(weights, axis=0), preferred_element_type=jnp.float32
            )
    lane = lax.broadcasted_iota(jnp.int32, (1, lanes), 1)
    factors = jnp.zeros((1, lanes), jnp.float32)
    for p in range(n_p):
        factors = jnp.where(lane // n_i == p, metric_ref[assign_ref[p]], factors)
    first = (lax.axis_index("orb") * row_blocks + block0 + step) * tile
    row = first + lax.broadcasted_iota(jnp.int32, (tile, lanes), 0)
    out_ref[...] = jnp.where(row < n_basis, total * factors, 0.0).astype(out_ref.dtype)


def transform(build, block0, n_blocks, n_basis, scalars, table, b_tiles):
    n_p, _, slots, tile, _ = b_tiles.shape
    n_i = scalars[0].shape[0]
    lanes = n_p * n_i
    blocks = (n_basis + tile - 1) // tile
    smem = pl.BlockSpec(memory_space=pltpu.SMEM)
    vmem = pl.BlockSpec(memory_space=pltpu.VMEM)
    hbm = pl.BlockSpec(memory_space=pl.ANY)
    out_shape = [jax.ShapeDtypeStruct((n_blocks * tile, lanes), jnp.bfloat16)]
    out_specs = [pl.BlockSpec((tile, lanes), lambda m: (m, 0))]
    scratch = [
        pltpu.VMEM((n_p, 16, lanes), jnp.bfloat16),
        pltpu.VMEM((n_blocks, n_p, slots, tile, tile), b_tiles.dtype),
        pltpu.SemaphoreType.DMA((n_blocks, n_p)),
    ]
    if build:
        out_shape.append(jax.ShapeDtypeStruct(((blocks + 1) * tile, lanes), jnp.bfloat16))
        out_specs.append(vmem)
        scratch += [
            pltpu.VMEM((n_i, 8, n_basis), jnp.bfloat16),
            pltpu.SemaphoreType.DMA((n_i,)),
        ]
    return pl.pallas_call(
        functools.partial(transform_kernel, build, n_basis, block0),
        grid=(n_blocks,),
        out_shape=out_shape,
        in_specs=[smem] * len(scalars) + [hbm if build else vmem, hbm],
        out_specs=out_specs,
        scratch_shapes=scratch,
        compiler_params=pltpu.CompilerParams(vmem_limit_bytes=TRANSFORM_VMEM_BYTES),
        cost_estimate=pl.CostEstimate(
            flops=2 * n_blocks * n_p * slots * tile * tile * lanes,
            bytes_accessed=2 * n_blocks * n_p * slots * tile * tile,
            transcendentals=0,
        ),
        name="transform_first" if build else "transform_rest",
    )(*scalars, table, b_tiles)


def place_of(plane_rows, mu_dev):
    per_orb = mu_dev // plane_rows
    z, x, core = lax.axis_index("aux"), lax.axis_index("orb"), lax.axis_index("occ")
    n_orb = lax.axis_size("orb")
    away = x - z // per_orb
    link = lax.rem(jnp.where(core == 0, away, -away) + n_orb, n_orb)
    return link, core, lax.rem(z, per_orb) * plane_rows


def stage_kernel(plane_rows, counts, *refs):
    *parts, out_ref = refs
    mu_dev = sum(p.shape[0] for p in parts[: counts[0]])
    _, _, first = place_of(plane_rows, mu_dev)
    used = 0
    for k, count in enumerate(counts):
        start = 0
        for part in parts[used : used + count]:
            size = part.shape[0]

            @pl.when((first >= start) & (first < start + size))
            def _():
                at = pl.ds(pl.multiple_of(first - start, plane_rows), plane_rows)
                out_ref[k * plane_rows : (k + 1) * plane_rows, :] = part[at, :]

            start += size
        used += count


def stage(slabs, plane_rows):
    vmem = pl.BlockSpec(memory_space=pltpu.VMEM)
    parts = [p for s in slabs for p in s]
    return pl.pallas_call(
        functools.partial(stage_kernel, plane_rows, tuple(len(s) for s in slabs)),
        out_shape=jax.ShapeDtypeStruct((len(slabs) * plane_rows, parts[0].shape[1]), parts[0].dtype),
        in_specs=[vmem] * len(parts),
        out_specs=vmem,
        compiler_params=pltpu.CompilerParams(vmem_limit_bytes=VMEM_BYTES),
        cost_estimate=pl.CostEstimate(flops=1000000, bytes_accessed=0, transcendentals=0),
        name="stage",
    )(*parts)


def choose_kernel(plane_rows, mu_dev, own_ref, came_ref, out_ref):
    link, _, _ = place_of(plane_rows, mu_dev)

    @pl.when(link == 0)
    def _():
        out_ref[...] = own_ref[...]

    @pl.when(link != 0)
    def _():
        out_ref[...] = came_ref[...]


def choose(own, came, plane_rows, mu_dev):
    vmem = pl.BlockSpec(memory_space=pltpu.VMEM)
    return pl.pallas_call(
        functools.partial(choose_kernel, plane_rows, mu_dev),
        out_shape=jax.ShapeDtypeStruct(own.shape, own.dtype),
        in_specs=[vmem] * 2,
        out_specs=vmem,
        compiler_params=pltpu.CompilerParams(vmem_limit_bytes=VMEM_BYTES),
        cost_estimate=pl.CostEstimate(flops=1000000, bytes_accessed=0, transcendentals=0),
        name="choose",
    )(own, came)


def accumulate_kernel(n_candidates, counts, has_prev, *refs):
    candidates = refs[:n_candidates]
    parts = refs[n_candidates : n_candidates + sum(counts)]
    rest = refs[n_candidates + sum(counts) :]
    prev, outs = (rest[:2], rest[2:]) if has_prev else (None, rest)
    slabs, used = [], 0
    for count in counts:
        slabs.append(parts[used : used + count])
        used += count
    n = len(slabs)
    mine, mu_dev = outs[0].shape
    plane_rows = candidates[0].shape[0] // n
    link, core, _ = place_of(plane_rows, mu_dev)
    groups = [range(j, min(j + 2, n)) for j in range(0, n, 2)]

    def rows_at(j, side):
        which = core if side == 0 else 1 - core
        at = pl.ds(pl.multiple_of(j * plane_rows + which * mine, mine), mine)
        c = [r[at, :] for r in candidates]
        if n_candidates == 2:
            return jnp.where(link < 2, c[0], c[1])
        return jnp.where(link < 2, jnp.where(link == 0, c[0], c[1]), jnp.where(link == 2, c[2], c[3]))

    left = [
        [jnp.concatenate([rows_at(j, side) for j in g], axis=1) for side in range(2)] for g in groups
    ]
    step = 256

    def cut(slab, start):
        for part in slab:
            if start < part.shape[0]:
                return part[start : start + step, :]
            start -= part.shape[0]

    for start in range(0, mu_dev, step):
        right = [jnp.concatenate([cut(slabs[j], start) for j in g], axis=1) for g in groups]
        for side in range(2):
            acc = prev[side][:, start : start + step] if has_prev else None
            for k in range(len(groups)):
                part = contract_last(left[k][side], right[k])
                acc = part if acc is None else acc + part
            outs[side][:, start : start + step] = acc


def accumulate(candidates, slabs, prev, block_rows, mu_dev):
    counts = tuple(len(s) for s in slabs)
    has_prev = prev is not None
    operands = list(candidates) + [p for s in slabs for p in s] + (list(prev) if has_prev else [])
    vmem = pl.BlockSpec(memory_space=pltpu.VMEM)
    flops = 2 * 2 * block_rows * mu_dev * len(slabs) * slabs[0][0].shape[1]
    return pl.pallas_call(
        functools.partial(accumulate_kernel, len(candidates), counts, has_prev),
        out_shape=[jax.ShapeDtypeStruct((block_rows, mu_dev), jnp.float32)] * 2,
        in_specs=[vmem] * len(operands),
        out_specs=[vmem] * 2,
        compiler_params=pltpu.CompilerParams(vmem_limit_bytes=VMEM_BYTES),
        cost_estimate=pl.CostEstimate(flops=flops, bytes_accessed=0, transcendentals=0),
        name="accumulate",
    )(*operands)


def per_device(b_tiles, nu_block, tile_mask, assignment, metric_factor, orbitals, occupied_index):
    row_blocks, tile_size = b_tiles.shape[1], b_tiles.shape[3]
    n_basis = orbitals.shape[1]
    padded = (n_basis + tile_size - 1) // tile_size * tile_size
    mu_dev = row_blocks * tile_size
    n_aux, n_orb, n_occ = lax.axis_size("aux"), lax.axis_size("orb"), lax.axis_size("occ")
    block_rows = padded // (n_aux * n_occ)
    plane_rows = block_rows * n_occ
    per_orb = mu_dev // plane_rows

    scalars = (
        occupied_index,
        nu_block.transpose(0, 2, 1),
        tile_mask.transpose(0, 2, 1),
        assignment,
        metric_factor,
    )
    low, table = transform(True, 0, row_blocks // 2, n_basis, scalars, orbitals, b_tiles)
    (high,) = transform(False, row_blocks // 2, row_blocks // 2, n_basis, scalars, table, b_tiles)

    swap = [(0, 1), (1, 0)]
    ring = [(2 * i, 2 * ((i + 1) % n_aux)) for i in range(n_aux)]
    ring += [(2 * i + 1, 2 * ((i - 1) % n_aux) + 1) for i in range(n_aux)]

    def forward(slab):
        got = []
        for part in slab:
            got.append(lax.ppermute(part, ("aux", "occ"), ring))
        return tuple(got)

    def along(payload, links):
        pairs = []
        for i in range(n_aux):
            for c, sign in ((0, 1), (1, -1)):
                for ends in links:
                    at = [(i * n_orb + (i // per_orb + sign * k) % n_orb) * 2 + c for k in ends]
                    pairs.append(tuple(at))
        return lax.ppermute(payload, ("aux", "orb", "occ"), pairs)

    a = (low, high)
    b = []
    for part in a:
        b.append(lax.ppermute(part, "occ", swap))
    steps = n_aux // 2
    batches, batch, sends = [], [a], []
    for t in range(1, steps + 1):
        a = forward(a)
        batch.append(a)
        if t < steps:
            b = forward(b)
            batch.append(b)
        if t in BATCH_ENDS or t == steps:
            own = stage(batch, plane_rows)
            if t < steps:
                first = along(own, [(0, 1)])
                both = choose(own, first, plane_rows, mu_dev)
                sends.append((both, along(both, [(0, 3), (1, 2)])))
            else:
                sends.append((own, *(along(own, [(0, j)]) for j in range(1, n_orb))))
            batches.append(batch)
            batch = []

    partial = None
    for candidates, slabs in zip(sends, batches, strict=True):
        partial = accumulate(candidates, slabs, partial, block_rows, mu_dev)
    mine, other = partial
    return mine + lax.ppermute(other, "occ", swap)


def solution(mesh):
    in_specs = (
        P(("grp", "aux"), "orb", None, None, None),
        P(("grp", "aux"), "orb", None),
        P(("grp", "aux"), "orb", None),
        P(("grp", "aux")),
        P("grp"),
        P("grp", None),
        P(("grp", "occ")),
    )
    out_specs = P(("grp", "aux", "occ"), "orb")

    return jax.shard_map(
        per_device, mesh=mesh, in_specs=in_specs, out_specs=out_specs, check_vma=False
    )
```
